32 devices in a mesh: mode: 8 (over z, y), row: 4 (over x, core).
Axes of the slice: x: 2, y: 2, z: 4, core: 2. Of those that a mesh axis runs over, the one named last changes fastest.
Arguments:
- density: float32 [2, 2048, 2048], P(None, 'row', 'mode'), may hold values from -6 to 6
- auxiliary: float32 [2048, 32, 2, 128], P('row', 'mode'), may hold values from -2 to 2
- hamiltonian: bfloat16 [2048, 2048], P('row'), as said below
- coupling: int32 [2, 128], replicated, may hold values from 0 to 2047, as said below
- lead_index: int32 [32], P('mode'), may hold values from 0 to 1
- mode_level: float32 [32], P('mode'), may hold values from -2 to 2
- mode_width: float32 [32], P('mode'), may hold values from 0.05 to 3
- residue: float32 [32, 2], P('mode'), may hold values from -4 to 4
- occupation: float32 [32], P('mode'), may hold values from 0 to 1
- lead_gamma: bfloat16 [2, 128, 128], replicated, may hold values from -0.5 to 0.5
Outputs:
- density_rate: float32 [2, 2048, 2048], P(None, 'row', 'mode')
- auxiliary_rate: float32 [2048, 32, 2, 128], P('row', 'mode')
The draws below stay inside these ranges and needn't reach their ends.
Inputs may be any that keep to these rules, and one draw needn't show every extreme that they name: `coupling`: all 256 entries are distinct orbitals. `hamiltonian`: Symmetric.
All inputs are finite; a program needn't handle non-finite values.
Results may differ from the reference program's by a relative error of at most 0.0044.
Values may be sent and summed in bfloat16 or wider, within the bound.
A program may use at most 128 MiB of HBM per device.

```python
import math
import jax
import jax.numpy as jnp
from jax import lax

N = 2048
NC = 128
LEADS = 2
MODE_DEV = 4
MODES = 32
N_MODE = 8


def draw_hamiltonian(key, part):
    values = jax.random.normal(key, (N, N), jnp.float32)
    symmetric = (values + values.T) * 0.5 ** 0.5 / math.sqrt(N)
    return symmetric.astype(jnp.bfloat16)


def draw_coupling(key, part):
    ordering = jax.random.permutation(jax.random.fold_in(key, 7), N)
    return ordering[:LEADS * NC].reshape(LEADS, NC).astype(jnp.int32)


def plant(drawn, stream_key, low, largest):
    dims = drawn.shape
    index_at = [jax.random.randint(jax.random.fold_in(stream_key, axis), (), 0, dims[axis]) for axis in range(len(dims))]
    drawn = drawn.at[tuple(index_at)].set(low)
    longest = dims.index(max(dims))
    index_at[longest] = (index_at[longest] + 1) % dims[longest]
    return drawn.at[tuple(index_at)].set(largest)


def shard_levels(stream_key, dims, split, low, largest):
    def one(position, parts):
        steps = jax.random.uniform(jax.random.fold_in(jax.random.fold_in(stream_key, 6), position), (parts,), jnp.float32, low / len(split), largest / len(split))
        return jnp.repeat(jnp.exp(steps), dims[position] // parts).reshape((-1,) + (1,) * (len(dims) - position - 1))

    factor_of = one(*split[0])
    for cut in split[1:]:
        factor_of = factor_of * one(*cut)
    return factor_of


def bell_draw(rng, shape, spread, limit, shards=(), held_as=jnp.bfloat16):
    level = shard_levels(rng, shape, shards, -0.22, 0.18) if shards else 1.0
    drawn = jax.random.normal(rng, shape, jnp.float32) * spread * level
    return jnp.minimum(jnp.maximum(drawn, -limit), limit).astype(held_as)


def setup_inputs(seed: int = 0) -> dict:
    key_of = jax.random.split(jax.random.key(seed), 11)
    return {
        "density": bell_draw(key_of[0], (2, N, N), 1.0, 6.0, ((1, 4), (2, 8)), jnp.float32),
        "auxiliary": bell_draw(key_of[1], (N, MODES, 2, NC), 0.3, 2.0, ((0, 4), (1, 8)), jnp.float32),
        "hamiltonian": draw_hamiltonian(jax.random.fold_in(key_of[10], 71), 0),
        "coupling": draw_coupling(jax.random.fold_in(key_of[10], 71), 0),
        "lead_index": plant(jax.random.randint(key_of[4], (MODES,), 0, LEADS), jax.random.fold_in(key_of[4], 1), 0, LEADS - 1).astype(jnp.int32),
        "mode_level": jnp.clip(jax.random.uniform(key_of[5], (MODES,), jnp.float32, -2.0, 2.0) * shard_levels(key_of[5], (MODES,), ((0, 8),), -0.4, 0.0), -2.0, 2.0),
        "mode_width": jnp.clip(jnp.exp(math.log(3.0) - 4.0943445 * jax.random.uniform(key_of[6], (MODES,), jnp.float32) ** shard_levels(key_of[6], (MODES,), ((0, 8),), -0.2, 0.2)), 0.05, 3.0),
        "residue": bell_draw(key_of[7], (MODES, 2), 1.0, 4.0, ((0, 8),), jnp.float32),
        "occupation": jnp.clip(1.0 * jax.random.uniform(key_of[8], (MODES,), jnp.float32) ** shard_levels(key_of[8], (MODES,), ((0, 8),), -0.2, 0.2), 0.0, 1.0),
        "lead_gamma": bell_draw(key_of[9], (LEADS, NC, NC), NC ** -0.5, 0.5),
    }


step_size = 0.1
highest = lax.Precision.HIGHEST


def rho_rates(state, hamiltonian, lead_sums, select):
    dens_b = state.astype(jnp.bfloat16)
    ham_rho = jnp.stack([jnp.dot(hamiltonian, dens_b[component], preferred_element_type=jnp.float32) for component in range(2)])
    rho_ham = jnp.stack([jnp.dot(dens_b[component], hamiltonian, preferred_element_type=jnp.float32) for component in range(2)])
    forward = jnp.stack([jnp.dot(lead_sums[:, component, :], select.T, precision=highest) for component in range(2)])
    commutator = ham_rho - rho_ham
    real_part = commutator[1] + forward[0] + forward[0].T
    imag_part = -commutator[0] + forward[1] - forward[1].T
    return jnp.stack([real_part, imag_part])


def source_terms(state, lead_gamma, flat_coupling):
    dens_b = state.astype(jnp.bfloat16)
    coupled_rho = jnp.take(dens_b, flat_coupling, axis=2).astype(jnp.float32).reshape(2, N, LEADS, NC)
    return jnp.einsum("cali,lij->calj", coupled_rho, lead_gamma.astype(jnp.float32))


def aux_rates(state_aux, hamiltonian, sources, gamma_rows, onehot, level, width, residue, occupation):
    ham_aux = jnp.dot(hamiltonian, state_aux.astype(jnp.bfloat16).reshape(N, -1), preferred_element_type=jnp.float32).reshape(state_aux.shape)
    picked = jnp.einsum("calj,kl->akcj", sources, onehot, precision=highest)
    picked_rows = jnp.einsum("alj,kl->akj", gamma_rows, onehot, precision=highest)
    driven = picked - occupation[None, :, None, None] * picked_rows[:, :, None, :]
    shifted = ham_aux - level[None, :, None, None] * state_aux
    decay = width[None, :, None]
    res_re = residue[:, 0][None, :, None]
    res_im = residue[:, 1][None, :, None]
    aux_re = shifted[:, :, 1, :] - decay * state_aux[:, :, 0, :] + res_re * driven[:, :, 0, :] - res_im * driven[:, :, 1, :]
    aux_im = -shifted[:, :, 0, :] - decay * state_aux[:, :, 1, :] + res_re * driven[:, :, 1, :] + res_im * driven[:, :, 0, :]
    return jnp.stack([aux_re, aux_im], axis=2)


def reference(density, auxiliary, hamiltonian, coupling, lead_index, mode_level, mode_width, residue, occupation, lead_gamma):
    flat_coupling = coupling.reshape(-1).astype(jnp.int32)
    select = (jnp.arange(N, dtype=jnp.int32)[:, None] == flat_coupling[None, :]).astype(jnp.float32)
    onehot = (lead_index[:, None] == jnp.arange(LEADS, dtype=jnp.int32)[None, :]).astype(jnp.float32)
    sums_first = jnp.einsum("akcj,kl->aclj", auxiliary, onehot, precision=highest).reshape(N, 2, LEADS * NC)
    first_rho = rho_rates(density, hamiltonian, sums_first, select)
    middle = density + 0.5 * step_size * first_rho
    src_first = source_terms(density, lead_gamma, flat_coupling)
    src_second = source_terms(middle, lead_gamma, flat_coupling)
    gamma_rows = jnp.einsum("alj,ljk->alk", select.reshape(N, LEADS, NC), lead_gamma.astype(jnp.float32), precision=highest)
    aux_blocks = auxiliary.reshape(N, N_MODE, MODE_DEV, 2, NC).transpose(1, 0, 2, 3, 4)

    def advance(total, inputs):
        aux_blk, hot_blk, lev_blk, wid_blk, res_blk, occ_blk = inputs
        first = aux_rates(aux_blk, hamiltonian, src_first, gamma_rows, hot_blk, lev_blk, wid_blk, res_blk, occ_blk)
        moved = aux_blk + 0.5 * step_size * first
        second = aux_rates(moved, hamiltonian, src_second, gamma_rows, hot_blk, lev_blk, wid_blk, res_blk, occ_blk)
        total = total + jnp.einsum("akcj,kl->aclj", moved, hot_blk, precision=highest).reshape(N, 2, LEADS * NC)
        return total, first + 2.0 * second

    inputs = (aux_blocks, onehot.reshape(N_MODE, MODE_DEV, LEADS), mode_level.reshape(N_MODE, MODE_DEV),
              mode_width.reshape(N_MODE, MODE_DEV), residue.reshape(N_MODE, MODE_DEV, 2), occupation.reshape(N_MODE, MODE_DEV))
    sums_second, blocks_out = lax.scan(advance, jnp.zeros((N, 2, LEADS * NC), jnp.float32), inputs)
    auxiliary_rate = blocks_out.transpose(1, 0, 2, 3, 4).reshape(N, N_MODE * MODE_DEV, 2, NC)
    second_rho = rho_rates(middle, hamiltonian, sums_second, select)
    return first_rho + 2.0 * second_rho, auxiliary_rate
```

```python
import functools

import jax
import jax.numpy as jnp
from jax import lax
from jax.experimental import pallas as pl
from jax.experimental.pallas import tpu as pltpu
from jax.sharding import PartitionSpec as P

step_size = 0.1
highest = lax.Precision.HIGHEST
MESH = pl.DeviceIdType.MESH
ANY = pl.BlockSpec(memory_space=pl.ANY)


class Gather:
    def __init__(self, axis, size, pieces, src, dst, stage, sems):
        self.axis, self.size, self.pieces = axis, size, pieces
        self.src, self.dst = src, dst
        self.stage = stage
        self.send, self.recv, self.local = sems
        self.me = lax.axis_index(axis)
        self.hi, self.lo = self.me // 2, self.me % 2
        self.length = size // 2

    def copy(self, source, slot, piece, kind, target):
        return pltpu.make_async_remote_copy(
            src_ref=source,
            dst_ref=self.dst(slot, piece),
            send_sem=self.send.at[kind, slot, piece],
            recv_sem=self.recv.at[slot, piece],
            device_id={self.axis: target},
            device_id_type=MESH,
        )

    def up(self, slot, source, piece):
        return self.copy(source, slot, piece, 0, self.me + 2)

    def down(self, slot, source, piece):
        return self.copy(source, slot, piece, 1, self.me - 2)

    def pair(self, slot, source, piece):
        return self.copy(source, slot, piece, 2, self.me + 1 - 2 * self.lo)

    def can_up(self, allowed=True):
        return pl.when(allowed & (self.hi < self.length - 1))

    def can_down(self, allowed=True):
        return pl.when(allowed & (self.hi > 0))

    def first(self):
        for piece in range(self.pieces):
            args = (self.me, self.src(piece), piece)
            self.can_up()(lambda: self.up(*args).start())
            self.can_down()(lambda: self.down(*args).start())
            self.pair(*args).start()

    def keep_load(self):
        for piece in range(self.pieces):
            pltpu.make_async_copy(self.src(piece), self.stage.at[piece], self.local.at[piece]).start()

    def keep_store(self):
        for piece in range(self.pieces):
            pltpu.make_async_copy(self.src(piece), self.stage.at[piece], self.local.at[piece]).wait()
            pltpu.make_async_copy(self.stage.at[piece], self.dst(self.me, piece), self.local.at[piece]).start()

    def keep_end(self):
        for piece in range(self.pieces):
            pltpu.make_async_copy(self.stage.at[piece], self.dst(self.me, piece), self.local.at[piece]).wait()

    def step(self, s):
        for piece in range(self.pieces):

            @pl.when(self.hi - 1 - s >= 0)
            def _():
                slot = self.me - 2 * (1 + s)
                args = (slot, self.dst(slot, piece), piece)
                self.pair(*args).wait_recv()
                self.can_up()(lambda: self.up(*args).start())
                self.pair(*args).start()

            @pl.when(self.hi + 1 + s < self.length)
            def _():
                slot = self.me + 2 * (1 + s)
                args = (slot, self.dst(slot, piece), piece)
                self.pair(*args).wait_recv()
                self.can_down()(lambda: self.down(*args).start())
                self.pair(*args).start()

    def finish(self):
        for line in range(self.length):
            for piece in range(self.pieces):
                slot = 2 * line + 1 - self.lo
                self.pair(slot, self.dst(slot, piece), piece).wait_recv()
        for line in range(self.length):
            for piece in range(self.pieces):
                slot = 2 * line + self.lo
                args = (slot, self.src(piece), piece)
                self.can_up(line <= self.hi)(lambda: self.up(*args).wait_send())
                self.can_down(line >= self.hi)(lambda: self.down(*args).wait_send())
                self.pair(*args).wait_send()


def exchange_kernel(n_mode, src_ref, out_ref, send, recv):
    me = lax.axis_index("mode")
    copies = []
    for d in range(1, n_mode):
        target = lax.rem(me + d, n_mode)
        origin = lax.rem(me + n_mode - d, n_mode)
        out = pltpu.make_async_remote_copy(
            src_ref=src_ref.at[target],
            dst_ref=out_ref.at[d - 1],
            send_sem=send.at[d - 1],
            recv_sem=recv.at[d - 1],
            device_id={"mode": target},
            device_id_type=MESH,
        )
        out.start()
        copies.append(out)
    for out in copies:
        out.wait()


def exchange(partial):
    n_mode = partial.shape[0]
    return pl.pallas_call(
        functools.partial(exchange_kernel, n_mode),
        out_shape=jax.ShapeDtypeStruct((n_mode - 1,) + partial.shape[1:], partial.dtype),
        in_specs=[ANY],
        out_specs=ANY,
        scratch_shapes=[
            pltpu.SemaphoreType.DMA((n_mode - 1,)),
            pltpu.SemaphoreType.DMA((n_mode - 1,)),
        ],
        compiler_params=pltpu.CompilerParams(has_side_effects=True),
    )(partial)


def gather_kernel(n_mode, n_row, wide, with_ham, *refs):
    n_in = 4 if with_ham else 3
    rho, aux, chunk = refs[:3]
    ham = refs[3] if with_ham else None
    panel, cols, aux_all, sums, cross = refs[n_in : n_in + 5]
    ham_all = refs[n_in + 5] if with_ham else None
    rest = refs[n_in + 5 + (1 if with_ham else 0) :]
    rho_stage, aux_stage, ham_stage, chunk_stage = rest[:4]
    sems = rest[4:]
    rows, columns = rho.shape[1], rho.shape[2]
    half = aux.shape[1]
    chunk_rows = chunk.shape[0]

    def panel_at(slot, piece):
        if wide:
            start = pl.multiple_of(slot * columns, columns)
            return panel.at[piece, :, pl.ds(start, columns)]
        return panel.at[slot, piece]

    def cols_at(slot, piece):
        return cols.at[piece, pl.ds(pl.multiple_of(slot * rows, rows), rows), :]

    def aux_at(slot, piece):
        return aux_all.at[pl.ds(pl.multiple_of(slot * rows + piece * half, half), half), :]

    def ham_at(slot, piece):
        return ham_all.at[pl.ds(pl.multiple_of(slot * rows, rows), rows), :]

    across = Gather("mode", n_mode, 2, lambda p: rho.at[p], panel_at, rho_stage.at[0], sems[0:3])
    down = Gather("row", n_row, 2, lambda p: rho.at[p], cols_at, rho_stage.at[1], sems[3:6])
    modes = Gather("row", n_row, 2, lambda p: aux.at[p], aux_at, aux_stage, sems[6:9])
    gathers = [across, down, modes]
    if with_ham:
        gathers.insert(2, Gather("row", n_row, 1, lambda p: ham, ham_at, ham_stage, sems[9:12]))
    chunk_send, chunk_recv, cross_send, cross_recv, chunk_local = sems[12:17]

    mode_me, row_me = lax.axis_index("mode"), lax.axis_index("row")
    per = columns // chunk_rows
    for g in gathers:
        g.first()
    for d in range(1, n_mode):
        target = lax.rem(mode_me + d, n_mode)
        pltpu.make_async_remote_copy(
            src_ref=chunk,
            dst_ref=sums.at[mode_me],
            send_sem=chunk_send.at[d - 1],
            recv_sem=chunk_recv.at[d - 1],
            device_id={"mode": target},
            device_id_type=MESH,
        ).start()
    wanted_by = (row_me * n_mode + mode_me) // per
    for d in range(1, n_row):
        pltpu.make_async_remote_copy(
            src_ref=chunk,
            dst_ref=cross.at[lax.rem(mode_me, per)],
            send_sem=cross_send.at[d - 1],
            recv_sem=cross_recv.at[lax.rem(mode_me, per)],
            device_id={"mode": wanted_by, "row": lax.rem(row_me + d, n_row)},
            device_id_type=MESH,
        ).start()
    for g in gathers:
        g.keep_load()
    pltpu.make_async_copy(chunk, chunk_stage, chunk_local).start()
    for g in gathers:
        g.keep_store()
    pltpu.make_async_copy(chunk, chunk_stage, chunk_local).wait()
    pltpu.make_async_copy(chunk_stage, sums.at[mode_me], chunk_local).start()

    across.step(0)
    for g in gathers[1:]:
        if g is not modes:
            for s in range(g.length - 1):
                g.step(s)
    if n_mode // 2 > 2:
        across.step(1)
    for s in range(modes.length - 1):
        modes.step(s)
    for s in range(2, across.length - 1):
        across.step(s)

    for g in gathers:
        g.keep_end()
        g.finish()
    pltpu.make_async_copy(chunk_stage, sums.at[mode_me], chunk_local).wait()
    for d in range(1, n_mode):
        origin = lax.rem(mode_me + n_mode - d, n_mode)
        pltpu.make_async_remote_copy(
            src_ref=chunk,
            dst_ref=sums.at[origin],
            send_sem=chunk_send.at[d - 1],
            recv_sem=chunk_recv.at[d - 1],
            device_id={"mode": origin},
            device_id_type=MESH,
        ).wait()
    other_row = lax.rem(row_me + 1, n_row)

    def cross_copy(slot, d):
        return pltpu.make_async_remote_copy(
            src_ref=chunk,
            dst_ref=cross.at[slot],
            send_sem=cross_send.at[d - 1],
            recv_sem=cross_recv.at[slot],
            device_id={"row": other_row},
            device_id_type=MESH,
        )

    for d in range(1, n_row):
        cross_copy(0, d).wait_send()

    @pl.when((mode_me * columns) // rows != row_me)
    def _():
        for slot in range(per):
            cross_copy(slot, 1).wait_recv()


def gather(n_mode, n_row, rho, aux, chunk, ham):
    _, rows, columns = rho.shape
    width = aux.shape[1]
    chunk_rows = chunk.shape[0]
    wide = columns % 128 == 0
    bf = jnp.bfloat16
    with_ham = ham is not None
    aux = aux.reshape(2, rows // 2, width)
    shapes = [
        (2, rows, n_mode * columns) if wide else (n_mode, 2, rows, columns),
        (2, n_row * rows, columns),
        (n_row * rows, width),
        (n_mode,) + chunk.shape,
        (columns // chunk_rows,) + chunk.shape,
    ]
    if with_ham:
        shapes.append((n_row * rows, columns))
    dma = pltpu.SemaphoreType.DMA

    def group(size, pieces):
        return [dma((3, size, pieces)), dma((size, pieces)), dma((pieces,))]

    return pl.pallas_call(
        functools.partial(gather_kernel, n_mode, n_row, wide, with_ham),
        out_shape=[jax.ShapeDtypeStruct(s, bf) for s in shapes],
        in_specs=[ANY] * (4 if with_ham else 3),
        out_specs=[ANY] * len(shapes),
        scratch_shapes=[
            pltpu.VMEM((2, 2, rows, columns), bf),
            pltpu.VMEM(aux.shape, bf),
            pltpu.VMEM((1, rows, columns), bf),
            pltpu.VMEM(chunk.shape, bf),
        ]
        + group(n_mode, 2)
        + group(n_row, 2)
        + group(n_row, 2)
        + group(n_row, 1)
        + [
            dma((n_mode - 1,)),
            dma((n_mode - 1,)),
            dma((n_row - 1,)),
            dma((columns // chunk_rows,)),
            dma,
        ],
        compiler_params=pltpu.CompilerParams(has_side_effects=True),
    )(*((rho, aux, chunk, ham) if with_ham else (rho, aux, chunk)))


def shards(
    n_mode,
    n_row,
    density,
    auxiliary,
    hamiltonian,
    coupling,
    lead_index,
    mode_level,
    mode_width,
    residue,
    occupation,
    lead_gamma,
):
    bf, f32 = jnp.bfloat16, jnp.float32
    rows = density.shape[1]
    columns = density.shape[2]
    lead_count, coupled = coupling.shape
    local_modes = auxiliary.shape[1]
    mode_me, row_me = lax.axis_index("mode"), lax.axis_index("row")
    row_start = row_me * rows
    col_start = mode_me * columns
    chunk_rows = rows // n_mode
    flat = coupling.reshape(-1)
    pairs = lead_count * coupled
    own_columns = lax.dynamic_slice_in_dim(hamiltonian, col_start, columns, 1)
    row_select = (row_start + jnp.arange(rows, dtype=jnp.int32)[:, None] == flat[None, :]).astype(bf)
    col_select = (col_start + jnp.arange(columns, dtype=jnp.int32)[:, None] == flat[None, :]).astype(bf)
    all_select = (jnp.arange(n_mode * columns, dtype=jnp.int32)[:, None] == flat[None, :]).astype(bf)
    onehot = (lead_index[:, None] == jnp.arange(lead_count, dtype=jnp.int32)[None, :]).astype(f32)
    gamma_rows = [
        jnp.dot(
            row_select[:, l * coupled : (l + 1) * coupled], lead_gamma[l], preferred_element_type=f32
        )
        for l in range(lead_count)
    ]
    cross_row = col_start // rows
    cross_chunk = lax.rem(mode_me, rows // columns) * (columns // chunk_rows)

    def lead_partial(state_aux):
        leads = []
        for l in range(lead_count):
            total = 0.0
            for k in range(local_modes):
                total = total + onehot[k, l] * state_aux[:, k]
            leads.append(total)
        return jnp.stack(leads, axis=2).reshape(n_mode, chunk_rows, 2 * pairs)

    def reduced(state_aux):
        partial = lead_partial(state_aux)
        own = lax.dynamic_index_in_dim(partial, mode_me, 0, keepdims=False)
        others = exchange(partial.astype(bf))
        return (own + jnp.sum(others.astype(f32), axis=0)).astype(bf)

    def rates(state_rho, state_aux, ham_all):
        rho_b = state_rho.astype(bf)
        aux_b = state_aux.astype(bf).reshape(rows, -1)
        chunk = reduced(state_aux)
        out = gather(n_mode, n_row, rho_b, aux_b, chunk, own_columns if ham_all is None else None)
        panel, cols, aux_all, sums, cross = out[:5]
        if ham_all is None:
            ham_all = out[5]
        if panel.ndim == 4:
            panel = panel.transpose(1, 2, 0, 3)
        panel = panel.reshape(2 * rows, -1)
        ham_aux = jnp.dot(hamiltonian, aux_all, preferred_element_type=f32)
        ham_rho = [jnp.dot(hamiltonian, cols[c], preferred_element_type=f32) for c in range(2)]
        rho_ham = jnp.dot(panel, ham_all, preferred_element_type=f32)
        coupled_rho = jnp.dot(panel, all_select, preferred_element_type=f32).astype(bf)
        sources = [
            jnp.dot(
                coupled_rho[:, l * coupled : (l + 1) * coupled], lead_gamma[l], preferred_element_type=f32
            )
            for l in range(lead_count)
        ]
        own = lax.dynamic_slice_in_dim(sums, cross_chunk, columns // chunk_rows, 0)
        cross = jnp.where(cross_row == row_me, own, cross).reshape(columns, 2 * pairs)
        sums = sums.reshape(rows, 2 * pairs)
        contract = (((1,), (1,)), ((), ()))
        forward = [
            lax.dot_general(
                sums[:, c * pairs : (c + 1) * pairs], col_select, contract, preferred_element_type=f32
            )
            for c in range(2)
        ]
        backward = [
            lax.dot_general(
                row_select, cross[:, c * pairs : (c + 1) * pairs], contract, preferred_element_type=f32
            )
            for c in range(2)
        ]
        rho_rate = jnp.stack(
            [
                ham_rho[1] - rho_ham[rows:] + forward[0] + backward[0],
                rho_ham[:rows] - ham_rho[0] + forward[1] - backward[1],
            ]
        )
        ham_aux = ham_aux.reshape(rows, local_modes, 2, coupled)
        pieces = []
        for k in range(local_modes):
            driven = []
            grow = sum(onehot[k, l] * gamma_rows[l] for l in range(lead_count))
            for c in range(2):
                src = sum(onehot[k, l] * sources[l][c * rows : (c + 1) * rows] for l in range(lead_count))
                driven.append(src)
            driven[0] = driven[0] - occupation[k] * grow
            driven[1] = driven[1] - occupation[k] * grow
            re, im = state_aux[:, k, 0], state_aux[:, k, 1]
            shift_re = ham_aux[:, k, 0] - mode_level[k] * re
            shift_im = ham_aux[:, k, 1] - mode_level[k] * im
            w_re, w_im = residue[k, 0], residue[k, 1]
            pieces.append(shift_im - mode_width[k] * re + w_re * driven[0] - w_im * driven[1])
            pieces.append(-shift_re - mode_width[k] * im + w_re * driven[1] + w_im * driven[0])
        aux_rate = jnp.stack(pieces, axis=1).reshape(state_aux.shape)
        return rho_rate, aux_rate, ham_all

    first_rho, first_aux, ham_all = rates(density, auxiliary, None)
    middle_rho = density + 0.5 * step_size * first_rho
    middle_aux = auxiliary + 0.5 * step_size * first_aux
    second_rho, second_aux, _ = rates(middle_rho, middle_aux, ham_all)
    return (first_rho + 2.0 * second_rho, first_aux + 2.0 * second_aux)


def solution(mesh):
    in_specs = (
        P(None, "row", "mode"),
        P("row", "mode", None, None),
        P("row", None),
        P(),
        P("mode"),
        P("mode"),
        P("mode"),
        P("mode", None),
        P("mode"),
        P(),
    )
    out_specs = (P(None, "row", "mode"), P("row", "mode", None, None))
    body = functools.partial(shards, mesh.shape["mode"], mesh.shape["row"])
    return jax.shard_map(body, mesh=mesh, in_specs=in_specs, out_specs=out_specs, check_vma=False)
```

```python
import functools

import jax
import jax.numpy as jnp
from jax import lax
from jax.experimental import pallas as pl
from jax.experimental.pallas import tpu as pltpu
from jax.sharding import PartitionSpec as P

step_size = 0.1
highest = lax.Precision.HIGHEST
MESH = pl.DeviceIdType.MESH
ANY = pl.BlockSpec(memory_space=pl.ANY)


class Gather:
    def __init__(self, axis, size, pieces, src, dst, stage, sems):
        self.axis, self.size, self.pieces = axis, size, pieces
        self.src, self.dst = src, dst
        self.stage = stage
        self.send, self.recv, self.local = sems
        self.me = lax.axis_index(axis)
        self.hi, self.lo = self.me // 2, self.me % 2
        self.length = size // 2

    def copy(self, source, slot, piece, kind, target):
        return pltpu.make_async_remote_copy(
            src_ref=source,
            dst_ref=self.dst(slot, piece),
            send_sem=self.send.at[kind, slot, piece],
            recv_sem=self.recv.at[slot, piece],
            device_id={self.axis: target},
            device_id_type=MESH,
        )

    def up(self, slot, source, piece):
        return self.copy(source, slot, piece, 0, self.me + 2)

    def down(self, slot, source, piece):
        return self.copy(source, slot, piece, 1, self.me - 2)

    def pair(self, slot, source, piece):
        return self.copy(source, slot, piece, 2, self.me + 1 - 2 * self.lo)

    def can_up(self, allowed=True):
        return pl.when(allowed & (self.hi < self.length - 1))

    def can_down(self, allowed=True):
        return pl.when(allowed & (self.hi > 0))

    def first(self):
        for piece in range(self.pieces):
            args = (self.me, self.src(piece), piece)
            self.can_up()(lambda: self.up(*args).start())
            self.can_down()(lambda: self.down(*args).start())
            self.pair(*args).start()

    def keep_load(self):
        for piece in range(self.pieces):
            pltpu.make_async_copy(self.src(piece), self.stage.at[piece], self.local.at[piece]).start()

    def keep_store(self):
        for piece in range(self.pieces):
            pltpu.make_async_copy(self.src(piece), self.stage.at[piece], self.local.at[piece]).wait()
            pltpu.make_async_copy(self.stage.at[piece], self.dst(self.me, piece), self.local.at[piece]).start()

    def keep_end(self):
        for piece in range(self.pieces):
            pltpu.make_async_copy(self.stage.at[piece], self.dst(self.me, piece), self.local.at[piece]).wait()

    def step(self, s):
        for piece in range(self.pieces):

            @pl.when(self.hi - 1 - s >= 0)
            def _():
                slot = self.me - 2 * (1 + s)
                args = (slot, self.dst(slot, piece), piece)
                self.pair(*args).wait_recv()
                self.can_up()(lambda: self.up(*args).start())
                self.pair(*args).start()

            @pl.when(self.hi + 1 + s < self.length)
            def _():
                slot = self.me + 2 * (1 + s)
                args = (slot, self.dst(slot, piece), piece)
                self.pair(*args).wait_recv()
                self.can_down()(lambda: self.down(*args).start())
                self.pair(*args).start()

    def finish(self):
        for line in range(self.length):
            for piece in range(self.pieces):
                slot = 2 * line + 1 - self.lo
                self.pair(slot, self.dst(slot, piece), piece).wait_recv()
        for line in range(self.length):
            for piece in range(self.pieces):
                slot = 2 * line + self.lo
                args = (slot, self.src(piece), piece)
                self.can_up(line <= self.hi)(lambda: self.up(*args).wait_send())
                self.can_down(line >= self.hi)(lambda: self.down(*args).wait_send())
                self.pair(*args).wait_send()


def exchange_kernel(n_mode, src_ref, out_ref, send, recv):
    me = lax.axis_index("mode")
    copies = []
    for d in range(1, n_mode):
        target = lax.rem(me + d, n_mode)
        origin = lax.rem(me + n_mode - d, n_mode)
        out = pltpu.make_async_remote_copy(
            src_ref=src_ref.at[target],
            dst_ref=out_ref.at[d - 1],
            send_sem=send.at[d - 1],
            recv_sem=recv.at[d - 1],
            device_id={"mode": target},
            device_id_type=MESH,
        )
        out.start()
        copies.append(out)
    for out in copies:
        out.wait()


def exchange(partial):
    n_mode = partial.shape[0]
    return pl.pallas_call(
        functools.partial(exchange_kernel, n_mode),
        out_shape=jax.ShapeDtypeStruct((n_mode - 1,) + partial.shape[1:], partial.dtype),
        in_specs=[ANY],
        out_specs=ANY,
        scratch_shapes=[
            pltpu.SemaphoreType.DMA((n_mode - 1,)),
            pltpu.SemaphoreType.DMA((n_mode - 1,)),
        ],
        compiler_params=pltpu.CompilerParams(has_side_effects=True),
    )(partial)


def gather_kernel(n_mode, n_row, wide, with_ham, *refs):
    n_in = 4 if with_ham else 3
    rho, aux, chunk = refs[:3]
    ham = refs[3] if with_ham else None
    panel, cols, aux_all, sums, cross = refs[n_in : n_in + 5]
    ham_all = refs[n_in + 5] if with_ham else None
    rest = refs[n_in + 5 + (1 if with_ham else 0) :]
    rho_stage, aux_stage, ham_stage, chunk_stage = rest[:4]
    sems = rest[4:]
    rows, columns = rho.shape[1], rho.shape[2]
    half = aux.shape[1]
    chunk_rows = chunk.shape[0]

    def panel_at(slot, piece):
        if wide:
            start = pl.multiple_of(slot * columns, columns)
            return panel.at[piece, :, pl.ds(start, columns)]
        return panel.at[slot, piece]

    def cols_at(slot, piece):
        return cols.at[piece, pl.ds(pl.multiple_of(slot * rows, rows), rows), :]

    def aux_at(slot, piece):
        return aux_all.at[pl.ds(pl.multiple_of(slot * rows + piece * half, half), half), :]

    def ham_at(slot, piece):
        return ham_all.at[pl.ds(pl.multiple_of(slot * rows, rows), rows), :]

    across = Gather("mode", n_mode, 2, lambda p: rho.at[p], panel_at, rho_stage.at[0], sems[0:3])
    down = Gather("row", n_row, 2, lambda p: rho.at[p], cols_at, rho_stage.at[1], sems[3:6])
    modes = Gather("row", n_row, 2, lambda p: aux.at[p], aux_at, aux_stage, sems[6:9])
    gathers = [across, down, modes]
    if with_ham:
        gathers.insert(2, Gather("row", n_row, 1, lambda p: ham, ham_at, ham_stage, sems[9:12]))
    chunk_send, chunk_recv, cross_send, cross_recv, chunk_local = sems[12:17]

    mode_me, row_me = lax.axis_index("mode"), lax.axis_index("row")
    per = columns // chunk_rows
    for g in gathers:
        g.first()
    for d in range(1, n_mode):
        target = lax.rem(mode_me + d, n_mode)
        pltpu.make_async_remote_copy(
            src_ref=chunk,
            dst_ref=sums.at[mode_me],
            send_sem=chunk_send.at[d - 1],
            recv_sem=chunk_recv.at[d - 1],
            device_id={"mode": target},
            device_id_type=MESH,
        ).start()
    wanted_by = (row_me * n_mode + mode_me) // per
    for d in range(1, n_row):
        pltpu.make_async_remote_copy(
            src_ref=chunk,
            dst_ref=cross.at[lax.rem(mode_me, per)],
            send_sem=cross_send.at[d - 1],
            recv_sem=cross_recv.at[lax.rem(mode_me, per)],
            device_id={"mode": wanted_by, "row": lax.rem(row_me + d, n_row)},
            device_id_type=MESH,
        ).start()
    for g in gathers:
        g.keep_load()
    pltpu.make_async_copy(chunk, chunk_stage, chunk_local).start()
    for g in gathers:
        g.keep_store()
    pltpu.make_async_copy(chunk, chunk_stage, chunk_local).wait()
    pltpu.make_async_copy(chunk_stage, sums.at[mode_me], chunk_local).start()

    across.step(0)
    for g in gathers[1:]:
        if g is not modes:
            for s in range(g.length - 1):
                g.step(s)
    if n_mode // 2 > 2:
        across.step(1)
    for s in range(modes.length - 1):
        modes.step(s)
    for s in range(2, across.length - 1):
        across.step(s)

    for g in gathers:
        g.keep_end()
        g.finish()
    pltpu.make_async_copy(chunk_stage, sums.at[mode_me], chunk_local).wait()
    for d in range(1, n_mode):
        origin = lax.rem(mode_me + n_mode - d, n_mode)
        pltpu.make_async_remote_copy(
            src_ref=chunk,
            dst_ref=sums.at[origin],
            send_sem=chunk_send.at[d - 1],
            recv_sem=chunk_recv.at[d - 1],
            device_id={"mode": origin},
            device_id_type=MESH,
        ).wait()
    other_row = lax.rem(row_me + 1, n_row)

    def cross_copy(slot, d):
        return pltpu.make_async_remote_copy(
            src_ref=chunk,
            dst_ref=cross.at[slot],
            send_sem=cross_send.at[d - 1],
            recv_sem=cross_recv.at[slot],
            device_id={"row": other_row},
            device_id_type=MESH,
        )

    for d in range(1, n_row):
        cross_copy(0, d).wait_send()

    @pl.when((mode_me * columns) // rows != row_me)
    def _():
        for slot in range(per):
            cross_copy(slot, 1).wait_recv()


def gather(n_mode, n_row, rho, aux, chunk, ham):
    _, rows, columns = rho.shape
    width = aux.shape[1]
    chunk_rows = chunk.shape[0]
    wide = columns % 128 == 0
    bf = jnp.bfloat16
    with_ham = ham is not None
    aux = aux.reshape(2, rows // 2, width)
    shapes = [
        (2, rows, n_mode * columns) if wide else (n_mode, 2, rows, columns),
        (2, n_row * rows, columns),
        (n_row * rows, width),
        (n_mode,) + chunk.shape,
        (columns // chunk_rows,) + chunk.shape,
    ]
    if with_ham:
        shapes.append((n_row * rows, columns))
    dma = pltpu.SemaphoreType.DMA

    def group(size, pieces):
        return [dma((3, size, pieces)), dma((size, pieces)), dma((pieces,))]

    return pl.pallas_call(
        functools.partial(gather_kernel, n_mode, n_row, wide, with_ham),
        out_shape=[jax.ShapeDtypeStruct(s, bf) for s in shapes],
        in_specs=[ANY] * (4 if with_ham else 3),
        out_specs=[ANY] * len(shapes),
        scratch_shapes=[
            pltpu.VMEM((2, 2, rows, columns), bf),
            pltpu.VMEM(aux.shape, bf),
            pltpu.VMEM((1, rows, columns), bf),
            pltpu.VMEM(chunk.shape, bf),
        ]
        + group(n_mode, 2)
        + group(n_row, 2)
        + group(n_row, 2)
        + group(n_row, 1)
        + [
            dma((n_mode - 1,)),
            dma((n_mode - 1,)),
            dma((n_row - 1,)),
            dma((columns // chunk_rows,)),
            dma,
        ],
        compiler_params=pltpu.CompilerParams(has_side_effects=True),
    )(*((rho, aux, chunk, ham) if with_ham else (rho, aux, chunk)))


def lead_partial(params, aux, local_modes, lead_count, coupled):
    out = []
    for c in range(2):
        for l in range(lead_count):
            total = params[0, 5 + l] * aux(0, c)
            for k in range(1, local_modes):
                total = total + params[k, 5 + l] * aux(k, c)
            out.append(total)
    return out


def prepare_kernel(sizes, params, density, aux, rho_b, aux_b, partial):
    local_modes, lead_count, coupled = sizes
    rho_b[...] = density[...].astype(rho_b.dtype)
    aux_b[...] = aux[...].astype(aux_b.dtype)

    def piece(k, c):
        start = (2 * k + c) * coupled
        return aux[:, start : start + coupled]

    for at, total in enumerate(lead_partial(params, piece, *sizes)):
        partial[:, at * coupled : (at + 1) * coupled] = total.astype(partial.dtype)


def stage_kernel(sizes, second, *refs):
    local_modes, lead_count, coupled = sizes
    (params, ham, aux_all, panel, ham_all, all_select, cols) = refs[:7]
    (gamma, row_select, col_select, sums, cross, aux) = refs[7:13]
    f32, bf = jnp.float32, jnp.bfloat16
    pairs = lead_count * coupled
    if second:
        first_rho, first_aux, rho_out, aux_out = refs[13:]
    else:
        density, rho_out, aux_out, rho_b, aux_b, partial = refs[13:]

    def dot(x, y):
        return jnp.dot(x, y, preferred_element_type=f32)

    def dot_t(x, y):
        return lax.dot_general(x, y, (((1,), (1,)), ((), ())), preferred_element_type=f32)

    h = ham[...]
    rates = []
    source = []
    for c in range(2):
        rho = panel[c]
        part = slice(c * pairs, (c + 1) * pairs)
        commutator = dot(h, cols[c]) - dot(rho, ham_all[...])
        forward = dot_t(sums[:, part], col_select[...])
        backward = dot_t(row_select[...], cross[:, part])
        rates.append((commutator, forward, backward))
        coupled_rho = dot(rho, all_select[...]).astype(bf)
        source.append(
            [dot(coupled_rho[:, l * coupled : (l + 1) * coupled], gamma[l]) for l in range(lead_count)]
        )
    rho_rate = (
        rates[1][0] + rates[0][1] + rates[0][2],
        rates[1][1] - rates[0][0] - rates[1][2],
    )
    for c in range(2):
        if second:
            rho_out[c] = first_rho[c] + 2.0 * rho_rate[c]
        else:
            rho_out[c] = rho_rate[c]
            rho_b[c] = (density[c] + 0.5 * step_size * rho_rate[c]).astype(bf)
    grow = [
        dot(row_select[:, l * coupled : (l + 1) * coupled], gamma[l]) for l in range(lead_count)
    ]
    totals = [[0.0] * lead_count for _ in range(2)]
    for k in range(local_modes):
        cut = [slice((2 * k + c) * coupled, (2 * k + c + 1) * coupled) for c in range(2)]
        both = slice(2 * k * coupled, 2 * (k + 1) * coupled)
        ham_aux = dot(h, aux_all[:, both])
        level, width, w_re, w_im, occ = [params[k, i] for i in range(5)]
        hot = [params[k, 5 + l] for l in range(lead_count)]
        state = []
        for c in range(2):
            value = aux[:, cut[c]]
            if second:
                value = value + 0.5 * step_size * first_aux[:, cut[c]]
            state.append(value)
        rows_gamma = sum(hot[l] * grow[l] for l in range(lead_count))
        b_re, b_im = [
            sum(hot[l] * source[c][l] for l in range(lead_count)) - occ * rows_gamma for c in range(2)
        ]
        shift_re = ham_aux[:, :coupled] - level * state[0]
        shift_im = ham_aux[:, coupled:] - level * state[1]
        rate = (
            shift_im - width * state[0] + w_re * b_re - w_im * b_im,
            w_re * b_im + w_im * b_re - shift_re - width * state[1],
        )
        for c in range(2):
            if second:
                aux_out[:, cut[c]] = first_aux[:, cut[c]] + 2.0 * rate[c]
            else:
                aux_out[:, cut[c]] = rate[c]
                middle = state[c] + 0.5 * step_size * rate[c]
                aux_b[:, cut[c]] = middle.astype(bf)
                for l in range(lead_count):
                    totals[c][l] = totals[c][l] + hot[l] * middle
    if not second:
        for c in range(2):
            for l in range(lead_count):
                start = c * pairs + l * coupled
                partial[:, start : start + coupled] = totals[c][l].astype(bf)


def blocked(rows, block, shape, dim):
    if dim is None:
        return pl.BlockSpec(shape, lambda i: (0,) * len(shape))
    sizes = tuple(block if d == dim else size for d, size in enumerate(shape))
    return pl.BlockSpec(sizes, lambda i: tuple(i if d == dim else 0 for d in range(len(shape))))


def call(kernel, rows, inputs, outputs):
    block = 128 if rows % 128 == 0 else rows
    in_specs = [
        pl.BlockSpec(memory_space=pltpu.SMEM) if dim == "smem" else blocked(rows, block, x.shape, dim)
        for x, dim in inputs
    ]
    return pl.pallas_call(
        kernel,
        grid=(rows // block,),
        out_shape=[jax.ShapeDtypeStruct(shape, dtype) for shape, dtype, _ in outputs],
        in_specs=in_specs,
        out_specs=[blocked(rows, block, shape, dim) for shape, _, dim in outputs],
        compiler_params=pltpu.CompilerParams(
            dimension_semantics=("arbitrary",), vmem_limit_bytes=56 * 2**20
        ),
    )(*[x for x, _ in inputs])


def shards(
    n_mode,
    n_row,
    density,
    auxiliary,
    hamiltonian,
    coupling,
    lead_index,
    mode_level,
    mode_width,
    residue,
    occupation,
    lead_gamma,
):
    bf, f32 = jnp.bfloat16, jnp.float32
    rows = density.shape[1]
    columns = density.shape[2]
    lead_count, coupled = coupling.shape
    local_modes = auxiliary.shape[1]
    mode_me, row_me = lax.axis_index("mode"), lax.axis_index("row")
    row_start = row_me * rows
    col_start = mode_me * columns
    chunk_rows = rows // n_mode
    flat = coupling.reshape(-1)
    pairs = lead_count * coupled
    own_columns = lax.dynamic_slice_in_dim(hamiltonian, col_start, columns, 1)
    row_select = (row_start + jnp.arange(rows, dtype=jnp.int32)[:, None] == flat[None, :]).astype(bf)
    col_select = (col_start + jnp.arange(columns, dtype=jnp.int32)[:, None] == flat[None, :]).astype(bf)
    all_select = (jnp.arange(n_mode * columns, dtype=jnp.int32)[:, None] == flat[None, :]).astype(bf)
    onehot = (lead_index[:, None] == jnp.arange(lead_count, dtype=jnp.int32)[None, :]).astype(f32)
    params = jnp.concatenate(
        [mode_level[:, None], mode_width[:, None], residue, occupation[:, None], onehot], axis=1
    )
    aux = auxiliary.reshape(rows, -1)
    width = aux.shape[1]
    sizes = (local_modes, lead_count, coupled)
    cross_row = col_start // rows
    cross_chunk = lax.rem(mode_me, rows // columns) * (columns // chunk_rows)

    rho_shape, aux_shape, sum_shape = density.shape, aux.shape, (rows, 2 * pairs)

    def moved(rho_b, aux_b, partial, ham):
        partial = partial.reshape(n_mode, chunk_rows, 2 * pairs)
        own = lax.dynamic_index_in_dim(partial, mode_me, 0, keepdims=False)
        others = exchange(partial)
        chunk = (own.astype(f32) + jnp.sum(others.astype(f32), axis=0)).astype(bf)
        out = gather(n_mode, n_row, rho_b, aux_b, chunk, ham)
        panel, cols, aux_all, sums, cross = out[:5]
        if panel.ndim == 4:
            panel = panel.transpose(1, 2, 0, 3).reshape(2, rows, -1)
        own = lax.dynamic_slice_in_dim(sums, cross_chunk, columns // chunk_rows, 0)
        cross = jnp.where(cross_row == row_me, own, cross).reshape(columns, 2 * pairs)
        return panel, cols, aux_all, sums.reshape(rows, 2 * pairs), cross, out[5:]

    def stage(second, ham_all, panel, cols, aux_all, sums, cross, extra, outputs):
        inputs = [
            (params, "smem"),
            (hamiltonian, 0),
            (aux_all, None),
            (panel, 1),
            (ham_all, None),
            (all_select, None),
            (cols, None),
            (lead_gamma, None),
            (row_select, 0),
            (col_select, None),
            (sums, 0),
            (cross, None),
            (aux, 0),
        ] + extra
        return call(functools.partial(stage_kernel, sizes, second), rows, inputs, outputs)

    rho_b, aux_b, partial = call(
        functools.partial(prepare_kernel, sizes),
        rows,
        [(params, "smem"), (density, 1), (aux, 0)],
        [(rho_shape, bf, 1), (aux_shape, bf, 0), (sum_shape, bf, 0)],
    )
    *blocks, extra = moved(rho_b, aux_b, partial, own_columns)
    ham_all = extra[0]
    first_rho, first_aux, rho_b, aux_b, partial = stage(
        False,
        ham_all,
        *blocks,
        [(density, 1)],
        [
            (rho_shape, f32, 1),
            (aux_shape, f32, 0),
            (rho_shape, bf, 1),
            (aux_shape, bf, 0),
            (sum_shape, bf, 0),
        ],
    )
    *blocks, _ = moved(rho_b, aux_b, partial, None)
    rho_out, aux_out = stage(
        True,
        ham_all,
        *blocks,
        [(first_rho, 1), (first_aux, 0)],
        [(rho_shape, f32, 1), (aux_shape, f32, 0)],
    )
    return rho_out, aux_out.reshape(auxiliary.shape)


def solution(mesh):
    in_specs = (
        P(None, "row", "mode"),
        P("row", "mode", None, None),
        P("row", None),
        P(),
        P("mode"),
        P("mode"),
        P("mode"),
        P("mode", None),
        P("mode"),
        P(),
    )
    out_specs = (P(None, "row", "mode"), P("row", "mode", None, None))
    body = functools.partial(shards, mesh.shape["mode"], mesh.shape["row"])
    return jax.shard_map(body, mesh=mesh, in_specs=in_specs, out_specs=out_specs, check_vma=False)
```

```python
import functools

import jax
import jax.numpy as jnp
from jax import lax
from jax.experimental import pallas as pl
from jax.experimental.pallas import tpu as pltpu
from jax.sharding import PartitionSpec as P

step_size = 0.1
highest = lax.Precision.HIGHEST
MESH = pl.DeviceIdType.MESH
ANY = pl.BlockSpec(memory_space=pl.ANY)


class Gather:
    def __init__(self, axis, size, pieces, src, dst, stage, sems):
        self.axis, self.size, self.pieces = axis, size, pieces
        self.src, self.dst = src, dst
        self.stage = stage
        self.send, self.recv, self.local = sems
        self.me = lax.axis_index(axis)
        self.hi, self.lo = self.me // 2, self.me % 2
        self.length = size // 2

    def copy(self, source, slot, piece, kind, target):
        return pltpu.make_async_remote_copy(
            src_ref=source,
            dst_ref=self.dst(slot, piece),
            send_sem=self.send.at[kind, slot, piece],
            recv_sem=self.recv.at[slot, piece],
            device_id={self.axis: target},
            device_id_type=MESH,
        )

    def up(self, slot, source, piece):
        return self.copy(source, slot, piece, 0, self.me + 2)

    def down(self, slot, source, piece):
        return self.copy(source, slot, piece, 1, self.me - 2)

    def pair(self, slot, source, piece):
        return self.copy(source, slot, piece, 2, self.me + 1 - 2 * self.lo)

    def can_up(self, allowed=True):
        return pl.when(allowed & (self.hi < self.length - 1))

    def can_down(self, allowed=True):
        return pl.when(allowed & (self.hi > 0))

    def first(self):
        for piece in range(self.pieces):
            args = (self.me, self.src(piece), piece)
            self.can_up()(lambda: self.up(*args).start())
            self.can_down()(lambda: self.down(*args).start())
            self.pair(*args).start()

    def keep_load(self):
        for piece in range(self.pieces):
            pltpu.make_async_copy(self.src(piece), self.stage.at[piece], self.local.at[piece]).start()

    def keep_store(self):
        for piece in range(self.pieces):
            pltpu.make_async_copy(self.src(piece), self.stage.at[piece], self.local.at[piece]).wait()
            pltpu.make_async_copy(self.stage.at[piece], self.dst(self.me, piece), self.local.at[piece]).start()

    def keep_end(self):
        for piece in range(self.pieces):
            pltpu.make_async_copy(self.stage.at[piece], self.dst(self.me, piece), self.local.at[piece]).wait()

    def step(self, s):
        for piece in range(self.pieces):

            @pl.when(self.hi - 1 - s >= 0)
            def _():
                slot = self.me - 2 * (1 + s)
                args = (slot, self.dst(slot, piece), piece)
                self.pair(*args).wait_recv()
                self.can_up()(lambda: self.up(*args).start())
                self.pair(*args).start()

            @pl.when(self.hi + 1 + s < self.length)
            def _():
                slot = self.me + 2 * (1 + s)
                args = (slot, self.dst(slot, piece), piece)
                self.pair(*args).wait_recv()
                self.can_down()(lambda: self.down(*args).start())
                self.pair(*args).start()

    def finish(self):
        for line in range(self.length):
            for piece in range(self.pieces):
                slot = 2 * line + 1 - self.lo
                self.pair(slot, self.dst(slot, piece), piece).wait_recv()
        for line in range(self.length):
            for piece in range(self.pieces):
                slot = 2 * line + self.lo
                args = (slot, self.src(piece), piece)
                self.can_up(line <= self.hi)(lambda: self.up(*args).wait_send())
                self.can_down(line >= self.hi)(lambda: self.down(*args).wait_send())
                self.pair(*args).wait_send()


def gather_kernel(n_mode, n_row, wide, with_ham, *refs):
    n_in = 4 if with_ham else 3
    rho, aux, partial = refs[:3]
    ham = refs[3] if with_ham else None
    panel, cols, aux_all, sums, cross = refs[n_in : n_in + 5]
    ham_all = refs[n_in + 5] if with_ham else None
    rest = refs[n_in + 5 + (1 if with_ham else 0) :]
    rho_stage, aux_stage, ham_stage, chunk_stage, parts = rest[:5]
    sems = rest[5:]
    rows, columns = rho.shape[1], rho.shape[2]
    half = aux.shape[1]
    chunk_rows = partial.shape[1]
    mode_me, row_me = lax.axis_index("mode"), lax.axis_index("row")

    def panel_at(slot, piece):
        if wide:
            start = pl.multiple_of(slot * columns, columns)
            return panel.at[piece, :, pl.ds(start, columns)]
        return panel.at[slot, piece]

    def cols_at(slot, piece):
        return cols.at[piece, pl.ds(pl.multiple_of(slot * rows, rows), rows), :]

    def aux_at(slot, piece):
        return aux_all.at[pl.ds(pl.multiple_of(slot * rows + piece * half, half), half), :]

    def ham_at(slot, piece):
        return ham_all.at[pl.ds(pl.multiple_of(slot * rows, rows), rows), :]

    def ham_own(piece):
        if wide:
            return ham.at[:, pl.ds(pl.multiple_of(mode_me * columns, columns), columns)]
        return ham

    across = Gather("mode", n_mode, 2, lambda p: rho.at[p], panel_at, rho_stage.at[0], sems[0:3])
    down = Gather("row", n_row, 2, lambda p: rho.at[p], cols_at, rho_stage.at[1], sems[3:6])
    modes = Gather("row", n_row, 2, lambda p: aux.at[p], aux_at, aux_stage, sems[6:9])
    gathers = [across, down, modes]
    if with_ham:
        gathers.insert(2, Gather("row", n_row, 1, ham_own, ham_at, ham_stage, sems[9:12]))
    part_send, part_recv, chunk_send, chunk_recv, cross_send, cross_recv, chunk_local = sems[12:19]
    per = columns // chunk_rows

    def part_copy(d):
        target = lax.rem(mode_me + d, n_mode)
        return pltpu.make_async_remote_copy(
            src_ref=partial.at[target],
            dst_ref=parts.at[d],
            send_sem=part_send.at[d - 1],
            recv_sem=part_recv.at[d - 1],
            device_id={"mode": target},
            device_id_type=MESH,
        )

    def chunk_copy(d, slot, target):
        return pltpu.make_async_remote_copy(
            src_ref=sums.at[mode_me],
            dst_ref=sums.at[slot],
            send_sem=chunk_send.at[d - 1],
            recv_sem=chunk_recv.at[d - 1],
            device_id={"mode": target},
            device_id_type=MESH,
        )

    def cross_copy(d, slot):
        return pltpu.make_async_remote_copy(
            src_ref=sums.at[mode_me],
            dst_ref=cross.at[slot],
            send_sem=cross_send.at[d - 1],
            recv_sem=cross_recv.at[slot],
            device_id={
                "mode": (row_me * n_mode + mode_me) // per,
                "row": lax.rem(row_me + d, n_row),
            },
            device_id_type=MESH,
        )

    for g in gathers:
        g.first()
    for d in range(1, n_mode):
        part_copy(d).start()
    for g in gathers:
        g.keep_load()
    own_part = pltpu.make_async_copy(partial.at[mode_me], parts.at[0], chunk_local)
    own_part.start()
    for g in gathers:
        g.keep_store()
    own_part.wait()

    across.step(0)
    for g in gathers[1:]:
        if g is not modes:
            for s in range(g.length - 1):
                g.step(s)
    total = parts[0].astype(jnp.float32)
    for d in range(1, n_mode):
        part_copy(d).wait_recv()
        total = total + parts[d].astype(jnp.float32)
    chunk_stage[...] = total.astype(chunk_stage.dtype)
    kept = pltpu.make_async_copy(chunk_stage, sums.at[mode_me], chunk_local)
    kept.start()
    kept.wait()
    for d in range(1, n_mode):
        chunk_copy(d, mode_me, lax.rem(mode_me + d, n_mode)).start()
    for d in range(1, n_row):
        cross_copy(d, lax.rem(mode_me, per)).start()
    if n_mode // 2 > 2:
        across.step(1)
    for s in range(modes.length - 1):
        modes.step(s)
    for s in range(2, across.length - 1):
        across.step(s)

    for g in gathers:
        g.keep_end()
        g.finish()
    for d in range(1, n_mode):
        part_copy(d).wait_send()
        origin = lax.rem(mode_me + n_mode - d, n_mode)
        chunk_copy(d, origin, origin).wait()
    for d in range(1, n_row):
        cross_copy(d, 0).wait_send()

    @pl.when((mode_me * columns) // rows != row_me)
    def _():
        for slot in range(per):
            cross_copy(1, slot).wait_recv()


def gather(n_mode, n_row, rho, aux, partial, ham):
    _, rows, columns = rho.shape
    width = aux.shape[1]
    chunk = jax.ShapeDtypeStruct(partial.shape[1:], partial.dtype)
    chunk_rows = chunk.shape[0]
    wide = columns % 128 == 0
    bf = jnp.bfloat16
    with_ham = ham is not None
    aux = aux.reshape(2, rows // 2, width)
    shapes = [
        (2, rows, n_mode * columns) if wide else (n_mode, 2, rows, columns),
        (2, n_row * rows, columns),
        (n_row * rows, width),
        (n_mode,) + chunk.shape,
        (columns // chunk_rows,) + chunk.shape,
    ]
    if with_ham:
        shapes.append((n_row * rows, columns))
    dma = pltpu.SemaphoreType.DMA

    def group(size, pieces):
        return [dma((3, size, pieces)), dma((size, pieces)), dma((pieces,))]

    return pl.pallas_call(
        functools.partial(gather_kernel, n_mode, n_row, wide, with_ham),
        out_shape=[jax.ShapeDtypeStruct(s, bf) for s in shapes],
        in_specs=[ANY] * (4 if with_ham else 3),
        out_specs=[ANY] * len(shapes),
        scratch_shapes=[
            pltpu.VMEM((2, 2, rows, columns), bf),
            pltpu.VMEM(aux.shape, bf),
            pltpu.VMEM((1, rows, columns), bf),
            pltpu.VMEM(chunk.shape, bf),
            pltpu.VMEM(partial.shape, bf),
        ]
        + group(n_mode, 2)
        + group(n_row, 2)
        + group(n_row, 2)
        + group(n_row, 1)
        + [
            dma((n_mode - 1,)),
            dma((n_mode - 1,)),
            dma((n_mode - 1,)),
            dma((n_mode - 1,)),
            dma((n_row - 1,)),
            dma((columns // chunk_rows,)),
            dma,
        ],
        compiler_params=pltpu.CompilerParams(has_side_effects=True),
    )(*((rho, aux, partial, ham) if with_ham else (rho, aux, partial)))


def lead_partial(params, aux, local_modes, lead_count, coupled):
    out = []
    for c in range(2):
        for l in range(lead_count):
            total = params[0, 5 + l] * aux(0, c)
            for k in range(1, local_modes):
                total = total + params[k, 5 + l] * aux(k, c)
            out.append(total)
    return out


def prepare_kernel(sizes, params, density, aux, rho_b, aux_b, partial):
    local_modes, lead_count, coupled = sizes
    rho_b[...] = density[...].astype(rho_b.dtype)
    aux_b[...] = aux[...].astype(aux_b.dtype)

    def piece(k, c):
        start = (2 * k + c) * coupled
        return aux[:, start : start + coupled]

    for at, total in enumerate(lead_partial(params, piece, *sizes)):
        partial[:, at * coupled : (at + 1) * coupled] = total.astype(partial.dtype)


def stage_kernel(sizes, second, *refs):
    local_modes, lead_count, coupled = sizes
    params, places, ham, aux_all, panel, ham_all, cols, gamma, flat, sums, cross, aux = refs[:12]
    all_select, col_select, cross_own = refs[-3:]
    refs = refs[:-3]
    f32, bf = jnp.float32, jnp.bfloat16
    pairs = lead_count * coupled
    if second:
        first_rho, first_aux, rho_out, aux_out = refs[12:]
    else:
        density, rho_out, aux_out, rho_b, aux_b, partial = refs[12:]

    def dot(x, y):
        return jnp.dot(x, y, preferred_element_type=f32)

    def dot_t(x, y):
        return lax.dot_general(x, y, (((1,), (1,)), ((), ())), preferred_element_type=f32)

    block = aux.shape[0]
    step = pl.program_id(0)
    row_start, col_start, own_cross, cross_start = [places[i] for i in range(4)]

    def select(start, count):
        at = start + lax.broadcasted_iota(jnp.int32, (count, flat.shape[1]), 0)
        return (at == flat[...]).astype(f32).astype(bf)

    @pl.when(step == 0)
    def _():
        all_select[...] = select(0, all_select.shape[0])
        col_select[...] = select(col_start, col_select.shape[0])

        @pl.when(own_cross == 1)
        def _():
            columns = cross.shape[0]
            cross_own[...] = sums[pl.ds(pl.multiple_of(cross_start, columns), columns), :]

        @pl.when(own_cross == 0)
        def _():
            cross_own[...] = cross[...]

    row_select = select(row_start + step * block, block)
    own_sums = sums[pl.ds(pl.multiple_of(step * block, block), block), :]
    h = ham[...]
    rates = []
    source = []
    for c in range(2):
        rho = panel[c]
        part = slice(c * pairs, (c + 1) * pairs)
        commutator = dot(h, cols[c]) - dot(rho, ham_all[...])
        forward = dot_t(own_sums[:, part], col_select[...])
        backward = dot_t(row_select, cross_own[:, part])
        rates.append((commutator, forward, backward))
        coupled_rho = dot(rho, all_select[...]).astype(bf)
        source.append(
            [dot(coupled_rho[:, l * coupled : (l + 1) * coupled], gamma[l]) for l in range(lead_count)]
        )
    rho_rate = (
        rates[1][0] + rates[0][1] + rates[0][2],
        rates[1][1] - rates[0][0] - rates[1][2],
    )
    for c in range(2):
        if second:
            rho_out[c] = first_rho[c] + 2.0 * rho_rate[c]
        else:
            rho_out[c] = rho_rate[c]
            rho_b[c] = (density[c] + 0.5 * step_size * rho_rate[c]).astype(bf)
    grow = [
        dot(row_select[:, l * coupled : (l + 1) * coupled], gamma[l]) for l in range(lead_count)
    ]
    totals = [[0.0] * lead_count for _ in range(2)]
    for k in range(local_modes):
        cut = [slice((2 * k + c) * coupled, (2 * k + c + 1) * coupled) for c in range(2)]
        both = slice(2 * k * coupled, 2 * (k + 1) * coupled)
        ham_aux = dot(h, aux_all[:, both])
        level, width, w_re, w_im, occ = [params[k, i] for i in range(5)]
        hot = [params[k, 5 + l] for l in range(lead_count)]
        state = []
        for c in range(2):
            value = aux[:, cut[c]]
            if second:
                value = value + 0.5 * step_size * first_aux[:, cut[c]]
            state.append(value)
        rows_gamma = sum(hot[l] * grow[l] for l in range(lead_count))
        b_re, b_im = [
            sum(hot[l] * source[c][l] for l in range(lead_count)) - occ * rows_gamma for c in range(2)
        ]
        shift_re = ham_aux[:, :coupled] - level * state[0]
        shift_im = ham_aux[:, coupled:] - level * state[1]
        rate = (
            shift_im - width * state[0] + w_re * b_re - w_im * b_im,
            w_re * b_im + w_im * b_re - shift_re - width * state[1],
        )
        for c in range(2):
            if second:
                aux_out[:, cut[c]] = first_aux[:, cut[c]] + 2.0 * rate[c]
            else:
                aux_out[:, cut[c]] = rate[c]
                middle = state[c] + 0.5 * step_size * rate[c]
                aux_b[:, cut[c]] = middle.astype(bf)
                for l in range(lead_count):
                    totals[c][l] = totals[c][l] + hot[l] * middle
    if not second:
        for c in range(2):
            for l in range(lead_count):
                start = c * pairs + l * coupled
                partial[:, start : start + coupled] = totals[c][l].astype(bf)


def blocked(rows, block, shape, dim):
    if dim is None:
        return pl.BlockSpec(shape, lambda i: (0,) * len(shape))
    sizes = tuple(block if d == dim else size for d, size in enumerate(shape))
    return pl.BlockSpec(sizes, lambda i: tuple(i if d == dim else 0 for d in range(len(shape))))


def call(kernel, rows, inputs, outputs, scratch=()):
    block = 128 if rows % 128 == 0 else rows
    in_specs = [
        pl.BlockSpec(memory_space=pltpu.SMEM) if dim == "smem" else blocked(rows, block, x.shape, dim)
        for x, dim in inputs
    ]
    return pl.pallas_call(
        kernel,
        grid=(rows // block,),
        out_shape=[jax.ShapeDtypeStruct(shape, dtype) for shape, dtype, _ in outputs],
        in_specs=in_specs,
        out_specs=[blocked(rows, block, shape, dim) for shape, _, dim in outputs],
        scratch_shapes=list(scratch),
        compiler_params=pltpu.CompilerParams(
            dimension_semantics=("arbitrary",), vmem_limit_bytes=56 * 2**20
        ),
    )(*[x for x, _ in inputs])


def shards(
    n_mode,
    n_row,
    density,
    auxiliary,
    hamiltonian,
    coupling,
    lead_index,
    mode_level,
    mode_width,
    residue,
    occupation,
    lead_gamma,
):
    bf, f32 = jnp.bfloat16, jnp.float32
    rows = density.shape[1]
    columns = density.shape[2]
    lead_count, coupled = coupling.shape
    local_modes = auxiliary.shape[1]
    mode_me, row_me = lax.axis_index("mode"), lax.axis_index("row")
    row_start = row_me * rows
    col_start = mode_me * columns
    chunk_rows = rows // n_mode
    flat = coupling.reshape(-1)
    pairs = lead_count * coupled
    own_columns = hamiltonian
    if columns % 128:
        own_columns = lax.dynamic_slice_in_dim(hamiltonian, col_start, columns, 1)
    onehot = (lead_index[:, None] == jnp.arange(lead_count, dtype=jnp.int32)[None, :]).astype(f32)
    params = jnp.concatenate(
        [mode_level[:, None], mode_width[:, None], residue, occupation[:, None], onehot], axis=1
    )
    aux = auxiliary.reshape(rows, -1)
    width = aux.shape[1]
    sizes = (local_modes, lead_count, coupled)
    cross_row = col_start // rows
    places = jnp.stack(
        [
            row_start,
            col_start,
            (cross_row == row_me).astype(jnp.int32),
            lax.rem(mode_me, rows // columns) * columns,
        ]
    )

    rho_shape, aux_shape, sum_shape = density.shape, aux.shape, (rows, 2 * pairs)

    def moved(rho_b, aux_b, partial, ham):
        partial = partial.reshape(n_mode, chunk_rows, 2 * pairs)
        out = gather(n_mode, n_row, rho_b, aux_b, partial, ham)
        panel, cols, aux_all, sums, cross = out[:5]
        if panel.ndim == 4:
            panel = panel.transpose(1, 2, 0, 3).reshape(2, rows, -1)
        cross = cross.reshape(columns, 2 * pairs)
        return panel, cols, aux_all, sums.reshape(rows, 2 * pairs), cross, out[5:]

    def stage(second, ham_all, panel, cols, aux_all, sums, cross, extra, outputs):
        inputs = [
            (params, "smem"),
            (places, "smem"),
            (hamiltonian, 0),
            (aux_all, None),
            (panel, 1),
            (ham_all, None),
            (cols, None),
            (lead_gamma, None),
            (flat[None, :], None),
            (sums, None),
            (cross, None),
            (aux, 0),
        ] + extra
        scratch = [
            pltpu.VMEM((n_mode * columns, pairs), bf),
            pltpu.VMEM((columns, pairs), bf),
            pltpu.VMEM((columns, 2 * pairs), bf),
        ]
        kernel = functools.partial(stage_kernel, sizes, second)
        return call(kernel, rows, inputs, outputs, scratch)

    rho_b, aux_b, partial = call(
        functools.partial(prepare_kernel, sizes),
        rows,
        [(params, "smem"), (density, 1), (aux, 0)],
        [(rho_shape, bf, 1), (aux_shape, bf, 0), (sum_shape, bf, 0)],
    )
    *blocks, extra = moved(rho_b, aux_b, partial, own_columns)
    ham_all = extra[0]
    first_rho, first_aux, rho_b, aux_b, partial = stage(
        False,
        ham_all,
        *blocks,
        [(density, 1)],
        [
            (rho_shape, f32, 1),
            (aux_shape, f32, 0),
            (rho_shape, bf, 1),
            (aux_shape, bf, 0),
            (sum_shape, bf, 0),
        ],
    )
    *blocks, _ = moved(rho_b, aux_b, partial, None)
    rho_out, aux_out = stage(
        True,
        ham_all,
        *blocks,
        [(first_rho, 1), (first_aux, 0)],
        [(rho_shape, f32, 1), (aux_shape, f32, 0)],
    )
    return rho_out, aux_out.reshape(auxiliary.shape)


def solution(mesh):
    in_specs = (
        P(None, "row", "mode"),
        P("row", "mode", None, None),
        P("row", None),
        P(),
        P("mode"),
        P("mode"),
        P("mode"),
        P("mode", None),
        P("mode"),
        P(),
    )
    out_specs = (P(None, "row", "mode"), P("row", "mode", None, None))
    body = functools.partial(shards, mesh.shape["mode"], mesh.shape["row"])
    return jax.shard_map(body, mesh=mesh, in_specs=in_specs, out_specs=out_specs, check_vma=False)
```

```python
import functools

import jax
import jax.numpy as jnp
from jax import lax
from jax.experimental import pallas as pl
from jax.experimental.pallas import tpu as pltpu
from jax.sharding import PartitionSpec as P

step_size = 0.1
highest = lax.Precision.HIGHEST
MESH = pl.DeviceIdType.MESH
ANY = pl.BlockSpec(memory_space=pl.ANY)


class Gather:
    def __init__(self, axis, size, pieces, src, dst, stage, sems):
        self.axis, self.size, self.pieces = axis, size, pieces
        self.src, self.dst = src, dst
        self.stage = stage
        self.send, self.recv, self.local = sems
        self.me = lax.axis_index(axis)
        self.hi, self.lo = self.me // 2, self.me % 2
        self.length = size // 2

    def copy(self, source, slot, piece, kind, target):
        return pltpu.make_async_remote_copy(
            src_ref=source,
            dst_ref=self.dst(slot, piece),
            send_sem=self.send.at[kind, slot, piece],
            recv_sem=self.recv.at[slot, piece],
            device_id={self.axis: target},
            device_id_type=MESH,
        )

    def up(self, slot, source, piece):
        return self.copy(source, slot, piece, 0, self.me + 2)

    def down(self, slot, source, piece):
        return self.copy(source, slot, piece, 1, self.me - 2)

    def pair(self, slot, source, piece):
        return self.copy(source, slot, piece, 2, self.me + 1 - 2 * self.lo)

    def can_up(self, allowed=True):
        return pl.when(allowed & (self.hi < self.length - 1))

    def can_down(self, allowed=True):
        return pl.when(allowed & (self.hi > 0))

    def first(self):
        for piece in range(self.pieces):
            args = (self.me, self.src(piece), piece)
            self.can_up()(lambda: self.up(*args).start())
            self.can_down()(lambda: self.down(*args).start())
            self.pair(*args).start()

    def keep_load(self):
        for piece in range(self.pieces):
            pltpu.make_async_copy(self.src(piece), self.stage.at[piece], self.local.at[piece]).start()

    def keep_store(self):
        for piece in range(self.pieces):
            pltpu.make_async_copy(self.src(piece), self.stage.at[piece], self.local.at[piece]).wait()
            pltpu.make_async_copy(self.stage.at[piece], self.dst(self.me, piece), self.local.at[piece]).start()

    def keep_end(self):
        for piece in range(self.pieces):
            pltpu.make_async_copy(self.stage.at[piece], self.dst(self.me, piece), self.local.at[piece]).wait()

    def step(self, s):
        for piece in range(self.pieces):

            @pl.when(self.hi - 1 - s >= 0)
            def _():
                slot = self.me - 2 * (1 + s)
                args = (slot, self.dst(slot, piece), piece)
                self.pair(*args).wait_recv()
                self.can_up()(lambda: self.up(*args).start())
                self.pair(*args).start()

            @pl.when(self.hi + 1 + s < self.length)
            def _():
                slot = self.me + 2 * (1 + s)
                args = (slot, self.dst(slot, piece), piece)
                self.pair(*args).wait_recv()
                self.can_down()(lambda: self.down(*args).start())
                self.pair(*args).start()

    def finish(self):
        for line in range(self.length):
            for piece in range(self.pieces):
                slot = 2 * line + 1 - self.lo
                self.pair(slot, self.dst(slot, piece), piece).wait_recv()
        for line in range(self.length):
            for piece in range(self.pieces):
                slot = 2 * line + self.lo
                args = (slot, self.src(piece), piece)
                self.can_up(line <= self.hi)(lambda: self.up(*args).wait_send())
                self.can_down(line >= self.hi)(lambda: self.down(*args).wait_send())
                self.pair(*args).wait_send()


def gather_kernel(n_mode, n_row, wide, with_ham, *refs):
    n_in = 4 if with_ham else 3
    rho, aux, partial = refs[:3]
    ham = refs[3] if with_ham else None
    panel, cols, aux_all, sums, cross = refs[n_in : n_in + 5]
    ham_all = refs[n_in + 5] if with_ham else None
    rest = refs[n_in + 5 + (1 if with_ham else 0) :]
    rho_stage, aux_stage, ham_stage, chunk_stage, parts, part_stage = rest[:6]
    sems = rest[6:]
    rows, columns = rho.shape[1], rho.shape[2]
    half = aux.shape[1]
    chunk_rows = partial.shape[1]
    mode_me, row_me = lax.axis_index("mode"), lax.axis_index("row")

    def panel_at(slot, piece):
        if wide:
            start = pl.multiple_of(slot * columns, columns)
            return panel.at[piece // 2, pl.ds(piece % 2 * half, half), pl.ds(start, columns)]
        return panel.at[slot, piece // 2, pl.ds(piece % 2 * half, half)]

    def cols_at(slot, piece):
        return cols.at[piece, pl.ds(pl.multiple_of(slot * rows, rows), rows), :]

    def aux_at(slot, piece):
        return aux_all.at[pl.ds(pl.multiple_of(slot * rows + piece * half, half), half), :]

    def ham_at(slot, piece):
        return ham_all.at[pl.ds(pl.multiple_of(slot * rows, rows), rows), :]

    def rho_at(piece):
        return rho.at[piece // 2, pl.ds(piece % 2 * half, half), :]

    def ham_own(piece):
        if wide:
            return ham.at[:, pl.ds(pl.multiple_of(mode_me * columns, columns), columns)]
        return ham

    across = Gather("mode", n_mode, 4, rho_at, panel_at, part_stage, sems[0:3])
    down = Gather("row", n_row, 2, lambda p: rho.at[p], cols_at, rho_stage, sems[3:6])
    modes = Gather("row", n_row, 2, lambda p: aux.at[p], aux_at, aux_stage, sems[6:9])
    gathers = [across, down, modes]
    if with_ham:
        gathers.insert(2, Gather("row", n_row, 1, ham_own, ham_at, ham_stage, sems[9:12]))
    part_send, part_recv, chunk_send, chunk_recv, cross_send, cross_recv, chunk_local = sems[12:19]
    per = columns // chunk_rows

    def part_copy(d):
        target = lax.rem(mode_me + d, n_mode)
        return pltpu.make_async_remote_copy(
            src_ref=partial.at[target],
            dst_ref=parts.at[d],
            send_sem=part_send.at[d - 1],
            recv_sem=part_recv.at[d - 1],
            device_id={"mode": target},
            device_id_type=MESH,
        )

    def chunk_copy(d, slot, target):
        return pltpu.make_async_remote_copy(
            src_ref=sums.at[mode_me],
            dst_ref=sums.at[slot],
            send_sem=chunk_send.at[d - 1],
            recv_sem=chunk_recv.at[d - 1],
            device_id={"mode": target},
            device_id_type=MESH,
        )

    def cross_copy(d, slot):
        return pltpu.make_async_remote_copy(
            src_ref=sums.at[mode_me],
            dst_ref=cross.at[slot],
            send_sem=cross_send.at[d - 1],
            recv_sem=cross_recv.at[slot],
            device_id={
                "mode": (row_me * n_mode + mode_me) // per,
                "row": lax.rem(row_me + d, n_row),
            },
            device_id_type=MESH,
        )

    for g in gathers:
        g.first()
    for d in range(1, n_mode):
        part_copy(d).start()
    for g in gathers:
        g.keep_load()
    own_part = pltpu.make_async_copy(partial.at[mode_me], parts.at[0], chunk_local)
    own_part.start()
    for g in gathers:
        g.keep_store()
    own_part.wait()

    across.step(0)
    for g in gathers[1:]:
        if g is not modes:
            for s in range(g.length - 1):
                g.step(s)
    total = parts[0].astype(jnp.float32)
    for d in range(1, n_mode):
        part_copy(d).wait_recv()
        total = total + parts[d].astype(jnp.float32)
    chunk_stage[...] = total.astype(chunk_stage.dtype)
    kept = pltpu.make_async_copy(chunk_stage, sums.at[mode_me], chunk_local)
    kept.start()
    kept.wait()
    for d in range(1, n_mode):
        chunk_copy(d, mode_me, lax.rem(mode_me + d, n_mode)).start()
    for d in range(1, n_row):
        cross_copy(d, lax.rem(mode_me, per)).start()
    if n_mode // 2 > 2:
        across.step(1)
    for s in range(modes.length - 1):
        modes.step(s)
    for s in range(2, across.length - 1):
        across.step(s)

    for g in gathers:
        g.keep_end()
        g.finish()
    for d in range(1, n_mode):
        part_copy(d).wait_send()
        origin = lax.rem(mode_me + n_mode - d, n_mode)
        chunk_copy(d, origin, origin).wait()
    for d in range(1, n_row):
        cross_copy(d, 0).wait_send()

    @pl.when((mode_me * columns) // rows != row_me)
    def _():
        for slot in range(per):
            cross_copy(1, slot).wait_recv()


def gather(n_mode, n_row, rho, aux, partial, ham):
    _, rows, columns = rho.shape
    width = aux.shape[1]
    chunk = jax.ShapeDtypeStruct(partial.shape[1:], partial.dtype)
    chunk_rows = chunk.shape[0]
    wide = columns % 128 == 0
    bf = jnp.bfloat16
    with_ham = ham is not None
    aux = aux.reshape(2, rows // 2, width)
    shapes = [
        (2, rows, n_mode * columns) if wide else (n_mode, 2, rows, columns),
        (2, n_row * rows, columns),
        (n_row * rows, width),
        (n_mode,) + chunk.shape,
        (columns // chunk_rows,) + chunk.shape,
    ]
    if with_ham:
        shapes.append((n_row * rows, columns))
    dma = pltpu.SemaphoreType.DMA

    def group(size, pieces):
        return [dma((3, size, pieces)), dma((size, pieces)), dma((pieces,))]

    return pl.pallas_call(
        functools.partial(gather_kernel, n_mode, n_row, wide, with_ham),
        out_shape=[jax.ShapeDtypeStruct(s, bf) for s in shapes],
        in_specs=[ANY] * (4 if with_ham else 3),
        out_specs=[ANY] * len(shapes),
        scratch_shapes=[
            pltpu.VMEM((2, rows, columns), bf),
            pltpu.VMEM(aux.shape, bf),
            pltpu.VMEM((1, rows, columns), bf),
            pltpu.VMEM(chunk.shape, bf),
            pltpu.VMEM(partial.shape, bf),
            pltpu.VMEM((4, rows // 2, columns), bf),
        ]
        + group(n_mode, 4)
        + group(n_row, 2)
        + group(n_row, 2)
        + group(n_row, 1)
        + [
            dma((n_mode - 1,)),
            dma((n_mode - 1,)),
            dma((n_mode - 1,)),
            dma((n_mode - 1,)),
            dma((n_row - 1,)),
            dma((columns // chunk_rows,)),
            dma,
        ],
        compiler_params=pltpu.CompilerParams(has_side_effects=True),
    )(*((rho, aux, partial, ham) if with_ham else (rho, aux, partial)))


def lead_partial(params, aux, local_modes, lead_count, coupled):
    out = []
    for c in range(2):
        for l in range(lead_count):
            total = params[0, 5 + l] * aux(0, c)
            for k in range(1, local_modes):
                total = total + params[k, 5 + l] * aux(k, c)
            out.append(total)
    return out


def prepare_kernel(sizes, params, density, aux, rho_b, aux_b, partial):
    local_modes, lead_count, coupled = sizes
    rho_b[...] = density[...].astype(rho_b.dtype)
    aux_b[...] = aux[...].astype(aux_b.dtype)

    def piece(k, c):
        start = (2 * k + c) * coupled
        return aux[:, start : start + coupled]

    for at, total in enumerate(lead_partial(params, piece, *sizes)):
        partial[:, at * coupled : (at + 1) * coupled] = total.astype(partial.dtype)


def stage_kernel(sizes, second, *refs):
    local_modes, lead_count, coupled = sizes
    params, places, ham, aux_all, panel, ham_all, cols, gamma, flat, sums, cross, aux = refs[:12]
    all_select, col_select, cross_own = refs[-3:]
    refs = refs[:-3]
    f32, bf = jnp.float32, jnp.bfloat16
    pairs = lead_count * coupled
    if second:
        first_rho, first_aux, rho_out, aux_out = refs[12:]
    else:
        density, rho_out, aux_out, rho_b, aux_b, partial = refs[12:]

    def dot(x, y):
        return jnp.dot(x, y, preferred_element_type=f32)

    def dot_t(x, y):
        return lax.dot_general(x, y, (((1,), (1,)), ((), ())), preferred_element_type=f32)

    block = aux.shape[0]
    step = pl.program_id(0)
    row_start, col_start, own_cross, cross_start = [places[i] for i in range(4)]

    def select(start, count):
        at = start + lax.broadcasted_iota(jnp.int32, (count, flat.shape[1]), 0)
        return (at == flat[...]).astype(f32).astype(bf)

    @pl.when(step == 0)
    def _():
        all_select[...] = select(0, all_select.shape[0])
        col_select[...] = select(col_start, col_select.shape[0])

        @pl.when(own_cross == 1)
        def _():
            columns = cross.shape[0]
            cross_own[...] = sums[pl.ds(pl.multiple_of(cross_start, columns), columns), :]

        @pl.when(own_cross == 0)
        def _():
            cross_own[...] = cross[...]

    row_select = select(row_start + step * block, block)
    own_sums = sums[pl.ds(pl.multiple_of(step * block, block), block), :]
    h = ham[...]
    rates = []
    source = []
    for c in range(2):
        rho = panel[c]
        part = slice(c * pairs, (c + 1) * pairs)
        commutator = dot(h, cols[c]) - dot(rho, ham_all[...])
        forward = dot_t(own_sums[:, part], col_select[...])
        backward = dot_t(row_select, cross_own[:, part])
        rates.append((commutator, forward, backward))
        coupled_rho = dot(rho, all_select[...]).astype(bf)
        source.append(
            [dot(coupled_rho[:, l * coupled : (l + 1) * coupled], gamma[l]) for l in range(lead_count)]
        )
    rho_rate = (
        rates[1][0] + rates[0][1] + rates[0][2],
        rates[1][1] - rates[0][0] - rates[1][2],
    )
    for c in range(2):
        if second:
            rho_out[c] = first_rho[c] + 2.0 * rho_rate[c]
        else:
            rho_out[c] = rho_rate[c]
            rho_b[c] = (density[c] + 0.5 * step_size * rho_rate[c]).astype(bf)
    grow = [
        dot(row_select[:, l * coupled : (l + 1) * coupled], gamma[l]) for l in range(lead_count)
    ]
    totals = [[0.0] * lead_count for _ in range(2)]
    for k in range(local_modes):
        cut = [slice((2 * k + c) * coupled, (2 * k + c + 1) * coupled) for c in range(2)]
        both = slice(2 * k * coupled, 2 * (k + 1) * coupled)
        ham_aux = dot(h, aux_all[:, both])
        level, width, w_re, w_im, occ = [params[k, i] for i in range(5)]
        hot = [params[k, 5 + l] for l in range(lead_count)]
        state = []
        for c in range(2):
            value = aux[:, cut[c]]
            if second:
                value = value + 0.5 * step_size * first_aux[:, cut[c]]
            state.append(value)
        rows_gamma = sum(hot[l] * grow[l] for l in range(lead_count))
        b_re, b_im = [
            sum(hot[l] * source[c][l] for l in range(lead_count)) - occ * rows_gamma for c in range(2)
        ]
        shift_re = ham_aux[:, :coupled] - level * state[0]
        shift_im = ham_aux[:, coupled:] - level * state[1]
        rate = (
            shift_im - width * state[0] + w_re * b_re - w_im * b_im,
            w_re * b_im + w_im * b_re - shift_re - width * state[1],
        )
        for c in range(2):
            if second:
                aux_out[:, cut[c]] = first_aux[:, cut[c]] + 2.0 * rate[c]
            else:
                aux_out[:, cut[c]] = rate[c]
                middle = state[c] + 0.5 * step_size * rate[c]
                aux_b[:, cut[c]] = middle.astype(bf)
                for l in range(lead_count):
                    totals[c][l] = totals[c][l] + hot[l] * middle
    if not second:
        for c in range(2):
            for l in range(lead_count):
                start = c * pairs + l * coupled
                partial[:, start : start + coupled] = totals[c][l].astype(bf)


def blocked(rows, block, shape, dim):
    if dim is None:
        return pl.BlockSpec(shape, lambda i: (0,) * len(shape))
    sizes = tuple(block if d == dim else size for d, size in enumerate(shape))
    return pl.BlockSpec(sizes, lambda i: tuple(i if d == dim else 0 for d in range(len(shape))))


def call(kernel, rows, inputs, outputs, scratch=()):
    block = 128 if rows % 128 == 0 else rows
    in_specs = [
        pl.BlockSpec(memory_space=pltpu.SMEM) if dim == "smem" else blocked(rows, block, x.shape, dim)
        for x, dim in inputs
    ]
    return pl.pallas_call(
        kernel,
        grid=(rows // block,),
        out_shape=[jax.ShapeDtypeStruct(shape, dtype) for shape, dtype, _ in outputs],
        in_specs=in_specs,
        out_specs=[blocked(rows, block, shape, dim) for shape, _, dim in outputs],
        scratch_shapes=list(scratch),
        compiler_params=pltpu.CompilerParams(
            dimension_semantics=("arbitrary",), vmem_limit_bytes=56 * 2**20
        ),
    )(*[x for x, _ in inputs])


def shards(
    n_mode,
    n_row,
    density,
    auxiliary,
    hamiltonian,
    coupling,
    lead_index,
    mode_level,
    mode_width,
    residue,
    occupation,
    lead_gamma,
):
    bf, f32 = jnp.bfloat16, jnp.float32
    rows = density.shape[1]
    columns = density.shape[2]
    lead_count, coupled = coupling.shape
    local_modes = auxiliary.shape[1]
    mode_me, row_me = lax.axis_index("mode"), lax.axis_index("row")
    row_start = row_me * rows
    col_start = mode_me * columns
    chunk_rows = rows // n_mode
    flat = coupling.reshape(-1)
    pairs = lead_count * coupled
    own_columns = hamiltonian
    if columns % 128:
        own_columns = lax.dynamic_slice_in_dim(hamiltonian, col_start, columns, 1)
    onehot = (lead_index[:, None] == jnp.arange(lead_count, dtype=jnp.int32)[None, :]).astype(f32)
    params = jnp.concatenate(
        [mode_level[:, None], mode_width[:, None], residue, occupation[:, None], onehot], axis=1
    )
    aux = auxiliary.reshape(rows, -1)
    width = aux.shape[1]
    sizes = (local_modes, lead_count, coupled)
    cross_row = col_start // rows
    places = jnp.stack(
        [
            row_start,
            col_start,
            (cross_row == row_me).astype(jnp.int32),
            lax.rem(mode_me, rows // columns) * columns,
        ]
    )

    rho_shape, aux_shape, sum_shape = density.shape, aux.shape, (rows, 2 * pairs)

    def moved(rho_b, aux_b, partial, ham):
        partial = partial.reshape(n_mode, chunk_rows, 2 * pairs)
        out = gather(n_mode, n_row, rho_b, aux_b, partial, ham)
        panel, cols, aux_all, sums, cross = out[:5]
        if panel.ndim == 4:
            panel = panel.transpose(1, 2, 0, 3).reshape(2, rows, -1)
        cross = cross.reshape(columns, 2 * pairs)
        return panel, cols, aux_all, sums.reshape(rows, 2 * pairs), cross, out[5:]

    def stage(second, ham_all, panel, cols, aux_all, sums, cross, extra, outputs):
        inputs = [
            (params, "smem"),
            (places, "smem"),
            (hamiltonian, 0),
            (aux_all, None),
            (panel, 1),
            (ham_all, None),
            (cols, None),
            (lead_gamma, None),
            (flat[None, :], None),
            (sums, None),
            (cross, None),
            (aux, 0),
        ] + extra
        scratch = [
            pltpu.VMEM((n_mode * columns, pairs), bf),
            pltpu.VMEM((columns, pairs), bf),
            pltpu.VMEM((columns, 2 * pairs), bf),
        ]
        kernel = functools.partial(stage_kernel, sizes, second)
        return call(kernel, rows, inputs, outputs, scratch)

    rho_b, aux_b, partial = call(
        functools.partial(prepare_kernel, sizes),
        rows,
        [(params, "smem"), (density, 1), (aux, 0)],
        [(rho_shape, bf, 1), (aux_shape, bf, 0), (sum_shape, bf, 0)],
    )
    *blocks, extra = moved(rho_b, aux_b, partial, own_columns)
    ham_all = extra[0]
    first_rho, first_aux, rho_b, aux_b, partial = stage(
        False,
        ham_all,
        *blocks,
        [(density, 1)],
        [
            (rho_shape, f32, 1),
            (aux_shape, f32, 0),
            (rho_shape, bf, 1),
            (aux_shape, bf, 0),
            (sum_shape, bf, 0),
        ],
    )
    *blocks, _ = moved(rho_b, aux_b, partial, None)
    rho_out, aux_out = stage(
        True,
        ham_all,
        *blocks,
        [(first_rho, 1), (first_aux, 0)],
        [(rho_shape, f32, 1), (aux_shape, f32, 0)],
    )
    return rho_out, aux_out.reshape(auxiliary.shape)


def solution(mesh):
    in_specs = (
        P(None, "row", "mode"),
        P("row", "mode", None, None),
        P("row", None),
        P(),
        P("mode"),
        P("mode"),
        P("mode"),
        P("mode", None),
        P("mode"),
        P(),
    )
    out_specs = (P(None, "row", "mode"), P("row", "mode", None, None))
    body = functools.partial(shards, mesh.shape["mode"], mesh.shape["row"])
    return jax.shard_map(body, mesh=mesh, in_specs=in_specs, out_specs=out_specs, check_vma=False)
```
